256 devices in a mesh: tok: 64 (over y, z, core), feat: 4 (over x).
Axes of the slice: x: 4, y: 4, z: 8, core: 2. Of those that a mesh axis runs over, the one named last changes fastest.
Arguments:
- first_acts: bfloat16 [81920, 3584], P('tok', 'feat'), may hold values from -6 to 6
- second_acts: bfloat16 [81920, 3584], P('tok', 'feat'), may hold values from -6 to 6
- start_dirs: bfloat16 [3584, 256], P('feat'), may hold values from -0.09375 to 0.09375
Outputs:
- first_dirs: bfloat16 [3584, 256], P('feat')
- second_dirs: bfloat16 [3584, 256], P('feat')
- correlation: float32 [256, 256], replicated
The draws below stay inside these ranges and needn't reach their ends.
All inputs are finite; a program needn't handle non-finite values.
Results may differ from the reference program's by a relative error of at most 0.006.
Values may be sent and summed in bfloat16 or wider, within the bound.
A program may use at most 128 MiB of HBM per device.

```python
import jax
import jax.numpy as jnp
from jax import lax

D = 3584
K = 256
ITERS = 2
TOKENS = 81920


def layer_draw(key, which):
    latent = jax.random.normal(jax.random.fold_in(key, 11), (TOKENS, K), jnp.float32)
    strength = jnp.exp(jax.random.uniform(jax.random.fold_in(key, 12), (K,), jnp.float32, jnp.log(0.3), jnp.log(1.5)))
    mixing = jax.random.normal(jax.random.fold_in(key, 13 + which), (K, D), jnp.float32) / jnp.sqrt(jnp.float32(K))
    noise = jax.random.normal(jax.random.fold_in(key, 21 + which), (TOKENS, D), jnp.float32)
    column = jnp.exp(jax.random.uniform(jax.random.fold_in(key, 31 + which), (D,), jnp.float32, 0.0, jnp.log(3.0)))
    shared = jnp.dot(latent * strength[None, :], mixing)
    values = (0.8 * shared + 0.6 * noise) * column[None, :] / jnp.sqrt(jnp.mean(column * column))
    return jnp.clip(values, -6.0, 6.0)


def draw_first_acts(key, part):
    return layer_draw(key, 0).astype(jnp.bfloat16)


def draw_second_acts(key, part):
    return layer_draw(key, 1).astype(jnp.bfloat16)


def steps_of(rng, dims, shards, smallest, high):
    def one(position, blocks):
        steps = jax.random.uniform(jax.random.fold_in(jax.random.fold_in(rng, 6), position), (blocks,), jnp.float32, smallest / len(shards), high / len(shards))
        return jnp.repeat(jnp.exp(steps), dims[position] // blocks).reshape((-1,) + (1,) * (len(dims) - position - 1))

    loudness = one(*shards[0])
    for cut in shards[1:]:
        loudness = loudness * one(*cut)
    return loudness


def scatter_about(stream_key, dims, width, bound, shards=(), kind=jnp.bfloat16):
    entries = width * jax.random.normal(stream_key, dims, jnp.float32)
    if shards:
        entries = entries * steps_of(stream_key, dims, shards, -0.22, 0.18)
    return jnp.clip(entries, -bound, bound).astype(kind)


def setup_inputs(seed: int = 0) -> dict:
    keys = jax.random.split(jax.random.key(seed), 4)
    return {
        "first_acts": draw_first_acts(jax.random.fold_in(keys[3], 71), 0),
        "second_acts": draw_second_acts(jax.random.fold_in(keys[3], 71), 0),
        "start_dirs": scatter_about(keys[2], (D, K), D ** -0.5, 0.09375, ((0, 4),)),
    }


def half_step(source, target, dirs, scale):
    z_rows = jnp.dot(source.astype(jnp.float32), dirs.astype(jnp.float32), preferred_element_type=jnp.float32).astype(jnp.bfloat16)
    gram = jnp.dot(z_rows.T.astype(jnp.float32), z_rows.astype(jnp.float32), preferred_element_type=jnp.float32) / TOKENS
    cross = jnp.dot(target.T.astype(jnp.float32), z_rows.astype(jnp.float32), preferred_element_type=jnp.float32) / TOKENS
    lower = jnp.linalg.cholesky(gram)
    solved = lax.linalg.triangular_solve(lower, cross, left_side=False, lower=True, transpose_a=True)
    return ((solved * scale[:, None]).astype(jnp.bfloat16), z_rows, lower)

def col_scale(acts):
    meansq = lax.optimization_barrier(jnp.sum(jnp.square(acts.astype(jnp.float32)), axis=0)) / TOKENS
    return jnp.sqrt(jnp.float32(D)) / (meansq + 0.5)

def reference(first_acts, second_acts, start_dirs):
    scale_first = col_scale(first_acts)
    scale_second = col_scale(second_acts)
    second = start_dirs
    for step in range(ITERS):
        first, z_second, lower_second = half_step(second_acts, first_acts, second, scale_first)
        second, z_first, lower_first = half_step(first_acts, second_acts, first, scale_second)
    z_last = jnp.dot(second_acts.astype(jnp.float32), second.astype(jnp.float32), preferred_element_type=jnp.float32).astype(jnp.bfloat16)
    gram_last = jnp.dot(z_last.T.astype(jnp.float32), z_last.astype(jnp.float32), preferred_element_type=jnp.float32) / TOKENS
    pair = jnp.dot(z_first.T.astype(jnp.float32), z_last.astype(jnp.float32), preferred_element_type=jnp.float32) / TOKENS
    lower_last = jnp.linalg.cholesky(gram_last)
    left = lax.linalg.triangular_solve(lower_first, pair, left_side=True, lower=True)
    correlation = lax.linalg.triangular_solve(lower_last, left, left_side=False, lower=True, transpose_a=True)
    return (first, second, correlation)
```

```python
import functools
import types

import jax
import jax.numpy as jnp
from jax import lax
from jax.experimental import pallas as pl
from jax.experimental.pallas import tpu as pltpu
from jax.sharding import Mesh
from jax.sharding import PartitionSpec as P

ITERS = 2
TOK = ("tok_0", "tok_1", "tok_2")
MESH = pl.DeviceIdType.MESH
HI = lax.Precision.HIGHEST
F32, BF16 = jnp.float32, jnp.bfloat16
PIECE = 16


def lane_of(tile, lane):
    return jnp.broadcast_to(tile[:, lane : lane + 1], (8, 128))


def row_of(tile, row):
    return jnp.broadcast_to(tile[row : row + 1, :], (8, 128))


def inverse_factor(block):
    sub = lax.broadcasted_iota(jnp.int32, (8, 128), 0)
    lane = lax.broadcasted_iota(jnp.int32, (8, 128), 1)
    n = 16
    left = [block[8 * i : 8 * i + 8, :] for i in range(n)]
    right = [jnp.where(lane == sub + 8 * i, 1.0, 0.0).astype(F32) for i in range(n)]
    for jb in range(n):
        col = {i: [lane_of(left[i], 8 * jb + k) for k in range(8)] for i in range(jb, n)}
        for k in range(8):
            head = col[jb][k]
            r = lax.rsqrt(row_of(head, k))
            rr = r * r
            row_l, row_r = row_of(left[jb], k), row_of(right[jb], k)
            for later in range(k + 1, 8):
                s = row_of(head, later)
                for i in range(jb, n):
                    col[i][later] = col[i][later] - (col[i][k] * s) * rr
            sl, sr = row_l * rr, row_r * rr
            low = jnp.where(sub > k, head, 0.0)
            left[jb] = jnp.where(sub == k, row_l * r, left[jb] - low * sl)
            right[jb] = jnp.where(sub == k, row_r * r, right[jb] - low * sr)
            for i in range(jb + 1, n):
                left[i] = left[i] - col[i][k] * sl
                right[i] = right[i] - col[i][k] * sr
    return jnp.concatenate(right, axis=0)


def mm(a, b, ca=1, cb=0, precision=HI):
    return lax.dot_general(
        a, b, (((ca,), (cb,)), ((), ())), precision=precision, preferred_element_type=F32
    )


def factor_into(g, blocks, low, inv):
    blocks[0] = g[0:128, 0:128]
    blocks[1] = g[128:256, 128:256]
    inv[0:128, 128:256] = jnp.zeros((128, 128), F32)

    def part(s, carry):
        blocks[s] = inverse_factor(blocks[s])

        @pl.when(s == 0)
        def _():
            p = mm(g[128:256, 0:128], blocks[0], 1, 1)
            low[...] = p
            blocks[1] = blocks[1] - mm(p, p, 1, 1)

        return carry

    lax.fori_loop(0, 2, part, 0)
    inv[0:128, 0:128] = blocks[0]
    inv[128:256, 128:256] = blocks[1]
    inv[128:256, 0:128] = -mm(blocks[1], mm(low[...], blocks[0]))


def solve_kernel(tokens, root, lane, g_ref, piece_ref, ss_ref, dirs_ref, inv_ref, blocks, low):
    factor_into(g_ref[...] * (1.0 / tokens), blocks, low, inv_ref)
    solved = mm(piece_ref[...] * (1.0 / tokens), inv_ref[...], 1, 1)
    scale = root / (ss_ref[:, lane : lane + 1] * (1.0 / tokens) + 0.5)
    dirs_ref[...] = (solved * scale).astype(BF16)


def final_kernel(tokens, g_ref, first_inv_ref, corr_ref, blocks, low, inv):
    factor_into(g_ref[0] * (1.0 / tokens), blocks, low, inv)
    left = mm(first_inv_ref[...], g_ref[1] * (1.0 / tokens))
    corr_ref[...] = mm(left, inv[...], 1, 1)


def in_vmem(n):
    return [pl.BlockSpec(memory_space=pltpu.VMEM)] * n


def factor_scratch():
    return [pltpu.VMEM((2, 128, 128), F32), pltpu.VMEM((128, 128), F32)]


def solve(tokens, root, lane, gram, piece, ss):
    k = gram.shape[-1]
    return pl.pallas_call(
        functools.partial(solve_kernel, tokens, root, lane),
        out_shape=(
            jax.ShapeDtypeStruct(piece.shape, BF16),
            jax.ShapeDtypeStruct((k, k), F32),
        ),
        in_specs=in_vmem(3),
        out_specs=tuple(in_vmem(2)),
        scratch_shapes=factor_scratch(),
        name="solve",
    )(gram, piece, ss)


def finish(tokens, grams, first_inv):
    k = first_inv.shape[-1]
    return pl.pallas_call(
        functools.partial(final_kernel, tokens),
        out_shape=jax.ShapeDtypeStruct((k, k), F32),
        in_specs=in_vmem(2),
        out_specs=in_vmem(1)[0],
        scratch_shapes=[*factor_scratch(), pltpu.VMEM((k, k), F32)],
        name="finish",
    )(grams, first_inv)


class Copies:
    def __init__(self):
        self.sends = []

    def put(self, src, dst, send, recv, device, when=None):
        copy = pltpu.make_async_remote_copy(
            src_ref=src, dst_ref=dst, send_sem=send, recv_sem=recv,
            device_id=device, device_id_type=MESH,
        )
        self.act(copy.start, when)
        self.sends.append((copy, when))

    def arrived(self, dst, send, recv, device, when=None):
        copy = pltpu.make_async_remote_copy(
            src_ref=dst, dst_ref=dst, send_sem=send, recv_sem=recv,
            device_id=device, device_id_type=MESH,
        )
        self.act(copy.wait_recv, when)

    def act(self, what, when):
        if when is None:
            what()
        else:
            pl.when(when)(what)

    def drain(self):
        for copy, when in self.sends:
            self.act(copy.wait_send, when)


def step_kernel(mode, names, *refs):
    ref = types.SimpleNamespace(**dict(zip(names, refs)))
    nx, ny, nz, nc = (lax.axis_size(a) for a in ("feat", "tok_0", "tok_1", "tok_2"))
    x, y, z, c = (lax.axis_index(a) for a in ("feat", "tok_0", "tok_1", "tok_2"))
    owners = nz - 1
    tokens = ref.src.shape[0]
    feats = ref.src.shape[1]
    per_y = owners * PIECE
    per_c = ny * per_y
    half, quarter = tokens // 2, tokens // 4
    k = 256
    ng = ref.gs.shape[0]

    def at(value, size, unit):
        return pl.ds(pl.multiple_of(value, unit), size)

    loads = []
    src_load = pltpu.make_async_copy(ref.src, ref.s, ref.load_sem.at[0])
    src_load.start()
    other = ref.tgt if mode != "last" else ref.first_t
    other_load = pltpu.make_async_copy(other, ref.u, ref.load_sem.at[1])
    other_load.start()

    plane = []
    for dx in range(nx):
        for dy in range(ny):
            for dc in range(nc):
                if dx or dy or dc:
                    plane.append((dx, dy, dc))

    def plane_peer(dx, dy, dc):
        return lax.rem(x + dx, nx), lax.rem(y + dy, ny), lax.rem(c + dc, nc)

    barrier = pltpu.get_barrier_semaphore()
    for d in plane:
        px, py, pc = plane_peer(*d)
        pl.semaphore_signal(
            barrier, inc=1, device_id={"feat": px, "tok_0": py, "tok_2": pc}, device_id_type=MESH
        )
    for d in range(1, nz):
        pl.semaphore_signal(
            barrier, inc=1, device_id={"tok_1": lax.rem(z + d, nz)}, device_id_type=MESH
        )
    pl.semaphore_wait(barrier, len(plane) + nz - 1)

    copies = Copies()

    if mode == "first":
        w = ref.dirs
    else:
        w = ref.w
        piece = ref.piece
        row = c * per_c + y * per_y
        owner = z < owners

        @pl.when(owner)
        def _():
            w[at(row + z * PIECE, PIECE, PIECE), :] = piece[...]

        for d in range(1, nz):
            copies.put(
                piece, w.at[at(row + lax.rem(z, owners) * PIECE, PIECE, PIECE)],
                ref.wz_s.at[d - 1], ref.wz_r.at[d - 1],
                {"tok_1": lax.rem(z + d, nz)}, owner,
            )
        for d in range(1, nz):
            sender = lax.rem(z + nz - d, nz)
            copies.arrived(
                w.at[at(row + lax.rem(sender, owners) * PIECE, PIECE, PIECE)],
                ref.wz_s.at[d - 1], ref.wz_r.at[d - 1], {"tok_1": sender}, sender < owners,
            )
        for d in range(1, ny):
            copies.put(
                w.at[at(row, per_y, PIECE)], w.at[at(row, per_y, PIECE)],
                ref.wy_s.at[d - 1], ref.wy_r.at[d - 1], {"tok_0": lax.rem(y + d, ny)},
            )
        for d in range(1, ny):
            sender = lax.rem(y + ny - d, ny)
            copies.arrived(
                w.at[at(c * per_c + sender * per_y, per_y, PIECE)],
                ref.wy_s.at[d - 1], ref.wy_r.at[d - 1], {"tok_0": sender},
            )
        for d in range(1, nc):
            copies.put(
                w.at[at(c * per_c, per_c, PIECE)], w.at[at(c * per_c, per_c, PIECE)],
                ref.wc_s.at[d - 1], ref.wc_r.at[d - 1], {"tok_2": lax.rem(c + d, nc)},
            )
        for d in range(1, nc):
            sender = lax.rem(c + nc - d, nc)
            copies.arrived(
                w.at[at(sender * per_c, per_c, PIECE)],
                ref.wc_s.at[d - 1], ref.wc_r.at[d - 1], {"tok_2": sender},
            )

    src_load.wait()
    part, out = ref.part, ref.out

    def project(i, carry):
        rows = at(i * quarter, quarter, 16)
        value = jnp.dot(ref.s[rows, :], w[...], preferred_element_type=F32)
        part[rows, :] = value
        out[0, rows, :] = value[:, 0:128].astype(BF16)
        out[1, rows, :] = value[:, 128:256].astype(BF16)
        return carry

    lax.fori_loop(0, 4, project, 0)

    near = x + 1 - 2 * lax.rem(x, 2)
    far = nx - 1 - x
    high, odd = x // 2, lax.rem(x, 2)
    plans = (
        (lax.rem(high + odd, 2), high, near, far),
        (high, odd, far, near),
    )
    zf = ref.z
    for i, (k1, k2, one, two) in enumerate(plans):
        copies.put(
            out.at[i, at((1 - k1) * half, half, 16)], ref.r1.at[i],
            ref.x_s.at[i, 0], ref.x_r.at[i, 0], {"feat": one},
        )
    other_load.wait()
    if mode == "first":
        for j in range(feats // 128):
            cols = slice(j * 128, j * 128 + 128)
            def square_sum(value):
                return jnp.sum(jnp.square(value.astype(F32)), axis=0, keepdims=True)
            first = square_sum(ref.u[:, cols])
            second = square_sum(ref.s[:, cols])
            upper = lax.broadcasted_iota(jnp.int32, (128, 128), 0) < 64
            both = jnp.where(upper, jnp.broadcast_to(first, (128, 128)), jnp.broadcast_to(second, (128, 128)))
            ref.sb[cols, :] = both.T
    for i, (k1, k2, one, two) in enumerate(plans):
        copies.arrived(ref.r1.at[i], ref.x_s.at[i, 0], ref.x_r.at[i, 0], {"feat": one})
        lanes = slice(i * 128, i * 128 + 128)
        give = (1 - k2) * quarter
        value = part[at(k1 * half + give, quarter, 16), lanes] + ref.r1[i, at(give, quarter, 16), :].astype(F32)
        ref.g2[i] = value.astype(BF16)
        copies.put(
            ref.g2.at[i], ref.r2.at[i], ref.x_s.at[i, 1], ref.x_r.at[i, 1], {"feat": two}
        )
    for i, (k1, k2, one, two) in enumerate(plans):
        lanes = slice(i * 128, i * 128 + 128)
        keep = k2 * quarter
        value = part[at(k1 * half + keep, quarter, 16), lanes] + ref.r1[i, at(keep, quarter, 16), :].astype(F32)
        copies.arrived(ref.r2.at[i], ref.x_s.at[i, 1], ref.x_r.at[i, 1], {"feat": two})
        mine = at(k1 * half + keep, quarter, 16)
        zf[i, mine, :] = (value + ref.r2[i].astype(F32)).astype(BF16)
        copies.put(
            zf.at[i, mine], zf.at[i, mine], ref.x_s.at[i, 2], ref.x_r.at[i, 2], {"feat": two}
        )
    for i, (k1, k2, one, two) in enumerate(plans):
        copies.arrived(
            zf.at[i, at(k1 * half + (1 - k2) * quarter, quarter, 16)],
            ref.x_s.at[i, 2], ref.x_r.at[i, 2], {"feat": two},
        )
        mine = at(k1 * half, half, 16)
        copies.put(
            zf.at[i, mine], zf.at[i, mine], ref.x_s.at[i, 3], ref.x_r.at[i, 3], {"feat": one}
        )
    for i, (k1, k2, one, two) in enumerate(plans):
        copies.arrived(
            zf.at[i, at((1 - k1) * half, half, 16)],
            ref.x_s.at[i, 3], ref.x_r.at[i, 3], {"feat": one},
        )

    zt = ref.zt
    for i in range(2):
        zt[i * 128 : i * 128 + 128, :] = zf[i].T
    gs = ref.gs
    rows = at(x * 64, 64, 16)
    lefts = [zt[rows, :]] + ([ref.u[rows, :]] if mode == "last" else [])
    for n, left in enumerate(lefts):
        for i in range(2):
            gs[n, :, i * 128 : i * 128 + 128] = jnp.dot(left, zf[i], preferred_element_type=F32)
    for d in range(1, nc):
        peer = lax.rem(c + d, nc)
        copies.put(
            gs.at[:, at(peer * 32, 32, 8)], ref.rgc.at[d - 1],
            ref.gc_s.at[d - 1], ref.gc_r.at[d - 1], {"tok_2": peer},
        )
    crossed = mode != "last"
    if crossed:
        cb = ref.cb
        for lo in range(0, feats, 256):
            hi = min(lo + 256, feats)
            value = jnp.dot(zt[...], ref.u[:, lo:hi], preferred_element_type=F32)
            cb[lo:hi, :] = value.T
        for d in range(1, nc):
            peer = lax.rem(c + d, nc)
            copies.put(
                cb.at[at(peer * per_c, per_c, PIECE)], ref.rcc.at[d - 1],
                ref.cc_s.at[d - 1], ref.cc_r.at[d - 1], {"tok_2": peer},
            )
            if mode == "first":
                copies.put(
                    ref.sb.at[at(peer * per_c, per_c, PIECE)], ref.rsc.at[d - 1],
                    ref.sc_s.at[d - 1], ref.sc_r.at[d - 1], {"tok_2": peer},
                )

    gram = gs[:, at(c * 32, 32, 8), :]
    for d in range(1, nc):
        sender = {"tok_2": lax.rem(c + nc - d, nc)}
        copies.arrived(ref.rgc.at[d - 1], ref.gc_s.at[d - 1], ref.gc_r.at[d - 1], sender)
        gram = gram + ref.rgc[d - 1]
    ref.gy[...] = gram
    for d in range(1, ny):
        peer = lax.rem(y + d, ny)
        copies.put(
            ref.gy.at[:, at(peer * 8, 8, 8)], ref.rgy.at[d - 1],
            ref.gy_s.at[d - 1], ref.gy_r.at[d - 1], {"tok_0": peer},
        )
    if crossed:
        own = at(c * per_c, per_c, PIECE)
        cross = cb[own, :]
        for d in range(1, nc):
            sender = {"tok_2": lax.rem(c + nc - d, nc)}
            copies.arrived(ref.rcc.at[d - 1], ref.cc_s.at[d - 1], ref.cc_r.at[d - 1], sender)
            cross = cross + ref.rcc[d - 1]
        ref.cy[...] = cross
        if mode == "first":
            sums = ref.sb[own, :]
            for d in range(1, nc):
                sender = {"tok_2": lax.rem(c + nc - d, nc)}
                copies.arrived(ref.rsc.at[d - 1], ref.sc_s.at[d - 1], ref.sc_r.at[d - 1], sender)
                sums = sums + ref.rsc[d - 1]
            ref.sy[...] = sums
        for d in range(1, ny):
            peer = lax.rem(y + d, ny)
            copies.put(
                ref.cy.at[at(peer * per_y, per_y, PIECE)], ref.rcy.at[d - 1],
                ref.cy_s.at[d - 1], ref.cy_r.at[d - 1], {"tok_0": peer},
            )
            if mode == "first":
                copies.put(
                    ref.sy.at[at(peer * per_y, per_y, PIECE)], ref.rsy.at[d - 1],
                    ref.sy_s.at[d - 1], ref.sy_r.at[d - 1], {"tok_0": peer},
                )
    gram = ref.gy[:, at(y * 8, 8, 8), :]
    for d in range(1, ny):
        sender = {"tok_0": lax.rem(y + ny - d, ny)}
        copies.arrived(ref.rgy.at[d - 1], ref.gy_s.at[d - 1], ref.gy_r.at[d - 1], sender)
        gram = gram + ref.rgy[d - 1]
    ref.gz[...] = gram
    for d in range(1, nz):
        copies.put(
            ref.gz, ref.rgz.at[d - 1], ref.gz_s.at[d - 1], ref.gz_r.at[d - 1],
            {"tok_1": lax.rem(z + d, nz)},
        )
    if crossed:
        own = at(y * per_y, per_y, PIECE)
        cross = ref.cy[own, :]
        for d in range(1, ny):
            sender = {"tok_0": lax.rem(y + ny - d, ny)}
            copies.arrived(ref.rcy.at[d - 1], ref.cy_s.at[d - 1], ref.cy_r.at[d - 1], sender)
            cross = cross + ref.rcy[d - 1]
        ref.cz[...] = cross
        if mode == "first":
            sums = ref.sy[own, :]
            for d in range(1, ny):
                sender = {"tok_0": lax.rem(y + ny - d, ny)}
                copies.arrived(ref.rsy.at[d - 1], ref.sy_s.at[d - 1], ref.sy_r.at[d - 1], sender)
                sums = sums + ref.rsy[d - 1]
            ref.sz[...] = sums
        for d in range(1, nz):
            peer = lax.rem(z + d, nz)
            rows = at(lax.rem(peer, owners) * PIECE, PIECE, PIECE)
            copies.put(
                ref.cz.at[rows], ref.rcz.at[d - 1],
                ref.cz_s.at[d - 1], ref.cz_r.at[d - 1], {"tok_1": peer}, peer < owners,
            )
            if mode == "first":
                copies.put(
                    ref.sz.at[rows], ref.rsz.at[d - 1],
                    ref.sz_s.at[d - 1], ref.sz_r.at[d - 1], {"tok_1": peer}, peer < owners,
                )

    gram = ref.gz[...]
    for d in range(1, nz):
        sender = {"tok_1": lax.rem(z + nz - d, nz)}
        copies.arrived(ref.rgz.at[d - 1], ref.gz_s.at[d - 1], ref.gz_r.at[d - 1], sender)
        gram = gram + ref.rgz[d - 1]

    def place(px, py, pc):
        return (px * nc + pc) * ny + py

    ga = ref.ga
    mine = place(x, y, c)
    ref.gm[...] = gram
    ga[mine] = gram
    for i, d in enumerate(plane):
        px, py, pc = plane_peer(*d)
        copies.put(
            ref.gm, ga.at[mine], ref.ga_s.at[i], ref.ga_r.at[i],
            {"feat": px, "tok_0": py, "tok_2": pc},
        )
    if crossed:
        @pl.when(z < owners)
        def _():
            rows = at(lax.rem(z, owners) * PIECE, PIECE, PIECE)
            cross = ref.cz[rows, :]
            for d in range(1, nz):
                sender = {"tok_1": lax.rem(z + nz - d, nz)}
                copies.arrived(ref.rcz.at[d - 1], ref.cz_s.at[d - 1], ref.cz_r.at[d - 1], sender)
                cross = cross + ref.rcz[d - 1]
            ref.cross[...] = cross
            if mode == "first":
                sums = ref.sz[rows, :]
                for d in range(1, nz):
                    sender = {"tok_1": lax.rem(z + nz - d, nz)}
                    copies.arrived(ref.rsz.at[d - 1], ref.sz_s.at[d - 1], ref.sz_r.at[d - 1], sender)
                    sums = sums + ref.rsz[d - 1]
                ref.ss[...] = sums

        @pl.when(z >= owners)
        def _():
            ref.cross[...] = jnp.zeros_like(ref.cross)
            if mode == "first":
                ref.ss[...] = jnp.zeros_like(ref.ss)

    if mode == "mid":
        ref.z_t[...] = zt[...]
    if mode != "first":
        ref.w_out[...] = w[...]
    for i, (dx, dy, dc) in enumerate(plane):
        px, py, pc = lax.rem(x + nx - dx, nx), lax.rem(y + ny - dy, ny), lax.rem(c + nc - dc, nc)
        copies.arrived(
            ga.at[place(px, py, pc)], ref.ga_s.at[i], ref.ga_r.at[i],
            {"feat": px, "tok_0": py, "tok_2": pc},
        )
    for g in range(nx * ny * nc):
        for n in range(ng):
            ref.gram[n, g * 8 : g * 8 + 8, :] = ga[g, n]
    copies.drain()


def step(mode, collective_id, source, target, dirs, sizes):
    nx, ny, nz, nc = sizes
    tokens, feats = source.shape
    k = 256
    owners = nz - 1
    per_y = owners * PIECE
    per_c = ny * per_y
    assert per_c * nc == feats and nx == 4
    ng = 2 if mode == "last" else 1
    half, quarter = tokens // 2, tokens // 4
    vmem, hbm = pl.BlockSpec(memory_space=pltpu.VMEM), pl.BlockSpec(memory_space=pl.ANY)
    dma = pltpu.SemaphoreType.DMA

    ins = [("src", hbm), ("first_t" if mode == "last" else "tgt", hbm)]
    ins.append(("dirs" if mode == "first" else "piece", vmem))
    outs = [("gram", (ng, k, k), F32)]
    if mode != "first":
        outs.append(("w_out", (feats, k), BF16))
    if mode != "last":
        outs.append(("cross", (PIECE, k), F32))
    if mode == "first":
        outs.append(("ss", (PIECE, 128), F32))
    if mode == "mid":
        outs.append(("z_t", (k, tokens), BF16))
    scratch = dict(
        s=pltpu.VMEM((tokens, feats), BF16),
        u=pltpu.VMEM(target.shape, BF16),
        load_sem=dma((2,)),
        part=pltpu.VMEM((tokens, k), F32),
        out=pltpu.VMEM((2, tokens, 128), BF16),
        z=pltpu.VMEM((2, tokens, 128), BF16),
        zt=pltpu.VMEM((k, tokens), BF16),
        r1=pltpu.VMEM((2, half, 128), BF16),
        g2=pltpu.VMEM((2, quarter, 128), BF16),
        r2=pltpu.VMEM((2, quarter, 128), BF16),
        x_s=dma((2, 4)),
        x_r=dma((2, 4)),
        gs=pltpu.VMEM((ng, 64, k), F32),
        rgc=pltpu.VMEM((nc - 1, ng, 32, k), F32),
        gy=pltpu.VMEM((ng, 32, k), F32),
        rgy=pltpu.VMEM((ny - 1, ng, 8, k), F32),
        gz=pltpu.VMEM((ng, 8, k), F32),
        rgz=pltpu.VMEM((nz - 1, ng, 8, k), F32),
        gm=pltpu.VMEM((ng, 8, k), F32),
        ga=pltpu.VMEM((nx * ny * nc, ng, 8, k), F32),
        gc_s=dma((nc - 1,)), gc_r=dma((nc - 1,)),
        gy_s=dma((ny - 1,)), gy_r=dma((ny - 1,)),
        gz_s=dma((nz - 1,)), gz_r=dma((nz - 1,)),
        ga_s=dma((nx * ny * nc - 1,)), ga_r=dma((nx * ny * nc - 1,)),
    )
    if mode != "first":
        scratch |= dict(
            w=pltpu.VMEM((feats, k), BF16),
            wz_s=dma((nz - 1,)), wz_r=dma((nz - 1,)),
            wy_s=dma((ny - 1,)), wy_r=dma((ny - 1,)),
            wc_s=dma((nc - 1,)), wc_r=dma((nc - 1,)),
        )
    kinds = []
    if mode != "last":
        kinds.append(("c", k, F32))
        scratch["cb"] = pltpu.VMEM((feats, k), F32)
    if mode == "first":
        kinds.append(("s", 128, F32))
        scratch["sb"] = pltpu.VMEM((feats, 128), F32)
    for name, lanes, kind in kinds:
        scratch |= {
            "r" + name + "c": pltpu.VMEM((nc - 1, per_c, lanes), kind),
            name + "y": pltpu.VMEM((per_c, lanes), kind),
            "r" + name + "y": pltpu.VMEM((ny - 1, per_y, lanes), kind),
            name + "z": pltpu.VMEM((per_y, lanes), F32),
            "r" + name + "z": pltpu.VMEM((nz - 1, PIECE, lanes), F32),
            name + "c_s": dma((nc - 1,)), name + "c_r": dma((nc - 1,)),
            name + "y_s": dma((ny - 1,)), name + "y_r": dma((ny - 1,)),
            name + "z_s": dma((nz - 1,)), name + "z_r": dma((nz - 1,)),
        }
    names = [n for n, _ in ins] + [n for n, _, _ in outs] + list(scratch)
    values = pl.pallas_call(
        functools.partial(step_kernel, mode, names),
        out_shape=tuple(jax.ShapeDtypeStruct(s, d) for _, s, d in outs),
        in_specs=[spec for _, spec in ins],
        out_specs=tuple(vmem for _ in outs),
        scratch_shapes=list(scratch.values()),
        compiler_params=pltpu.CompilerParams(collective_id=collective_id, has_side_effects=True),
        name="step_" + mode,
    )(source, target, dirs)
    return dict(zip([n for n, _, _ in outs], values))


def body(first_acts, second_acts, start_dirs):
    sizes = tuple(lax.axis_size(a) for a in ("feat", *TOK))
    tokens = float(first_acts.shape[0] * lax.axis_size(TOK))
    root = float(first_acts.shape[1] * sizes[0]) ** 0.5
    acts = (first_acts, second_acts)
    got = step("first", 0, second_acts, first_acts, start_dirs, sizes)
    ss = got["ss"]
    dirs = [None, None]
    for h in range(2 * ITERS):
        side = h % 2
        piece, inverse = solve(tokens, root, 64 * side, got["gram"][0], got["cross"], ss)
        if h < 2 * ITERS - 1:
            got = step("mid", 1, acts[side], acts[1 - side], piece, sizes)
        else:
            got = step("last", 2, second_acts, got["z_t"], piece, sizes)
        dirs[side] = got["w_out"]
    return (dirs[0], dirs[1], finish(tokens, got["gram"], inverse))


def solution(mesh):
    split = Mesh(
        mesh.devices.reshape(4, 8, 2, mesh.shape["feat"]), ("tok_0", "tok_1", "tok_2", "feat")
    )
    in_specs = (P(TOK, "feat"), P(TOK, "feat"), P("feat", None))
    out_specs = (P("feat", None), P("feat", None), P())
    return jax.shard_map(body, mesh=split, in_specs=in_specs, out_specs=out_specs, check_vma=False)
```

```python
import functools
import types

import jax
import jax.numpy as jnp
from jax import lax
from jax.experimental import pallas as pl
from jax.experimental.pallas import tpu as pltpu
from jax.sharding import Mesh
from jax.sharding import PartitionSpec as P

ITERS = 2
STEPS = 2 * ITERS
CHUNKS = 2
TOK = ("tok_0", "tok_1", "tok_2")
MESH = pl.DeviceIdType.MESH
HI = lax.Precision.HIGHEST
F32, BF16 = jnp.float32, jnp.bfloat16
PIECE = 16


def inverse_factor(block, between=None):
    n = block.shape[0]
    sub = lax.broadcasted_iota(jnp.int32, (8, n), 0)
    left = block
    right = jnp.where(
        lax.broadcasted_iota(jnp.int32, (n, n), 0) == lax.broadcasted_iota(jnp.int32, (n, n), 1), 1.0, 0.0
    ).astype(F32)
    done = []
    for j in range(0, n, 8):
        if between is not None and j == n // 2:
            between()
        head_l, head_r = left[0:8], right[0:8]
        rest_l, rest_r = left[8:], right[8:]
        more = j + 8 < n
        head = [jnp.broadcast_to(head_l[:, j + k : j + k + 1], (8, n)) for k in range(8)]
        if more:
            rest = [jnp.broadcast_to(rest_l[:, j + k : j + k + 1], rest_l.shape) for k in range(8)]
        for k in range(8):
            r = lax.rsqrt(head[k][k : k + 1, :])
            rr = r * r
            row_l, row_r = head_l[k : k + 1, :], head_r[k : k + 1, :]
            for later in range(k + 1, 8):
                s = head[k][later : later + 1, :]
                head[later] = head[later] - (head[k] * s) * rr
                if more:
                    rest[later] = rest[later] - (rest[k] * s) * rr
            sl, sr = row_l * rr, row_r * rr
            low = jnp.where(sub > k, head[k], 0.0)
            head_l = jnp.where(sub == k, row_l * r, head_l - low * sl)
            head_r = jnp.where(sub == k, row_r * r, head_r - low * sr)
            if more:
                rest_l = rest_l - rest[k] * sl
                rest_r = rest_r - rest[k] * sr
        done.append(head_r)
        left, right = rest_l, rest_r
    return jnp.concatenate(done, axis=0)


def mm(a, b, ca=1, cb=0, precision=HI):
    return lax.dot_general(
        a, b, (((ca,), (cb,)), ((), ())), precision=precision, preferred_element_type=F32
    )


def inverse_into(g, scale, inv, between=None):
    one = inverse_factor(g[0:128, 0:128] * scale)
    inv[0:128, 0:128] = one
    inv[0:128, 128:256] = jnp.zeros((128, 128), F32)
    p = mm(g[128:256, 0:128] * scale, one, 1, 1)
    inv[128:256, 0:128] = mm(p, one)
    two = inverse_factor(g[128:256, 128:256] * scale - mm(p, p, 1, 1), between)
    inv[128:256, 128:256] = two
    inv[128:256, 0:128] = -mm(two, inv[128:256, 0:128])


def split(value):
    high = value.astype(BF16)
    return high, (value - high.astype(F32)).astype(BF16)


class Copies:
    def __init__(self):
        self.sends = []

    def put(self, src, dst, send, recv, device, when=None):
        copy = pltpu.make_async_remote_copy(
            src_ref=src, dst_ref=dst, send_sem=send, recv_sem=recv,
            device_id=device, device_id_type=MESH,
        )
        self.act(copy.start, when)
        self.sends.append((copy, when))

    def arrived(self, dst, send, recv, device, when=None):
        copy = pltpu.make_async_remote_copy(
            src_ref=dst, dst_ref=dst, send_sem=send, recv_sem=recv,
            device_id=device, device_id_type=MESH,
        )
        self.act(copy.wait_recv, when)

    def act(self, what, when):
        if when is None:
            what()
        else:
            pl.when(when)(what)

    def drain(self):
        for copy, when in self.sends:
            self.act(copy.wait_send, when)


def kernel(names, total_tokens, root, *refs):
    ref = types.SimpleNamespace(**dict(zip(names, refs)))
    nx, ny, nz, nc = (lax.axis_size(a) for a in ("feat", *TOK))
    x, y, z, c = (lax.axis_index(a) for a in ("feat", *TOK))
    owners = nz - 1
    tokens, feats = ref.first_acts.shape
    per_y = owners * PIECE
    per_c = ny * per_y
    chunk = tokens // CHUNKS
    half, quarter = chunk // 2, chunk // 4
    count = 1.0 / total_tokens

    def at(value, size, unit):
        return pl.ds(pl.multiple_of(value, unit), size)

    loads = [
        pltpu.make_async_copy(ref.start_dirs, ref.w, ref.load_sem.at[0]),
        pltpu.make_async_copy(ref.second_acts, ref.acts.at[1], ref.load_sem.at[1]),
        pltpu.make_async_copy(ref.first_acts, ref.acts.at[0], ref.load_sem.at[2]),
    ]
    for load in loads:
        load.start()

    plane = [
        (dx, dy, dc)
        for dx in range(nx) for dy in range(ny) for dc in range(nc) if dx or dy or dc
    ]

    def on_plane(dx, dy, dc):
        px, py, pc = lax.rem(x + dx + nx, nx), lax.rem(y + dy + ny, ny), lax.rem(c + dc + nc, nc)
        return (px, py, pc), {"feat": px, "tok_0": py, "tok_2": pc}

    def place(px, py, pc):
        return (px * nc + pc) * ny + py

    def after(i, d, n):
        return lax.rem(i + d, n)

    def before(i, d, n):
        return lax.rem(i + n - d, n)

    barrier = pltpu.get_barrier_semaphore()
    for d in plane:
        pl.semaphore_signal(barrier, inc=1, device_id=on_plane(*d)[1], device_id_type=MESH)
    for d in range(1, nz):
        pl.semaphore_signal(barrier, inc=1, device_id={"tok_1": after(z, d, nz)}, device_id_type=MESH)
    pl.semaphore_wait(barrier, len(plane) + nz - 1)

    near = x + 1 - 2 * lax.rem(x, 2)
    far = nx - 1 - x
    high, odd = x // 2, lax.rem(x, 2)
    ways = ((lax.rem(high + odd, 2), high, near, far), (high, odd, far, near))
    plans = [(u * 2 + i, u * chunk, i, *ways[i]) for u in range(CHUNKS) for i in range(2)]

    def column_sums():
        for j in range(feats // 128):
            cols = slice(j * 128, j * 128 + 128)
            first, second = (
                jnp.sum(jnp.square(ref.acts[i, :, cols].astype(F32)), axis=0, keepdims=True)
                for i in range(2)
            )
            upper = lax.broadcasted_iota(jnp.int32, (128, 128), 0) < 64
            ref.sb[cols, :] = jnp.where(
                upper, jnp.broadcast_to(first, (128, 128)), jnp.broadcast_to(second, (128, 128))
            ).T

    def projected(h, source, zf, copies, first_time, beside):
        for u in range(CHUNKS):

            def project(i, carry):
                rows = at(u * chunk + i * half, half, 16)
                value = jnp.dot(source[rows, :], ref.w[...], preferred_element_type=F32)
                ref.part[rows, :] = value
                ref.out[0, rows, :] = value[:, 0:128].astype(BF16)
                ref.out[1, rows, :] = value[:, 128:256].astype(BF16)
                return carry

            lax.fori_loop(0, 2, project, 0)
            for p, base, i, k1, k2, one, two in plans[2 * u : 2 * u + 2]:
                copies.put(
                    ref.out.at[i, at(base + (1 - k1) * half, half, 16)], ref.r1.at[h, p],
                    ref.x_s.at[p, 0], ref.x_r.at[h, p, 0], {"feat": one},
                )
        beside()
        for p, base, i, k1, k2, one, two in plans:
            copies.arrived(ref.r1.at[h, p], ref.x_s.at[p, 0], ref.x_r.at[h, p, 0], {"feat": one})
            lanes = slice(i * 128, i * 128 + 128)
            give = (1 - k2) * quarter
            value = ref.part[at(base + k1 * half + give, quarter, 16), lanes]
            ref.g2[p] = (value + ref.r1[h, p, at(give, quarter, 16), :].astype(F32)).astype(BF16)
            copies.put(
                ref.g2.at[p], ref.r2.at[h, p], ref.x_s.at[p, 1], ref.x_r.at[h, p, 1], {"feat": two}
            )
        for p, base, i, k1, k2, one, two in plans:
            lanes = slice(i * 128, i * 128 + 128)
            keep = k2 * quarter
            mine = at(base + k1 * half + keep, quarter, 16)
            value = ref.part[mine, lanes] + ref.r1[h, p, at(keep, quarter, 16), :].astype(F32)
            copies.arrived(ref.r2.at[h, p], ref.x_s.at[p, 1], ref.x_r.at[h, p, 1], {"feat": two})
            zf[i, mine, :] = (value + ref.r2[h, p].astype(F32)).astype(BF16)
            copies.put(
                zf.at[i, mine], zf.at[i, mine], ref.x_s.at[p, 2], ref.x_r.at[h, p, 2], {"feat": two}
            )
        for p, base, i, k1, k2, one, two in plans:
            copies.arrived(
                zf.at[i, at(base + k1 * half + (1 - k2) * quarter, quarter, 16)],
                ref.x_s.at[p, 2], ref.x_r.at[h, p, 2], {"feat": two},
            )
            mine = at(base + k1 * half, half, 16)
            copies.put(
                zf.at[i, mine], zf.at[i, mine], ref.x_s.at[p, 3], ref.x_r.at[h, p, 3], {"feat": one}
            )
        for p, base, i, k1, k2, one, two in plans:
            copies.arrived(
                zf.at[i, at(base + (1 - k1) * half, half, 16)],
                ref.x_s.at[p, 3], ref.x_r.at[h, p, 3], {"feat": one},
            )

    def gram_rows(zf, lefts):
        for n, left in enumerate(lefts):
            for i in range(2):
                ref.gs[n, :, i * 128 : i * 128 + 128] = jnp.dot(left, zf[i], preferred_element_type=F32)

    def gram_to_core(h, ng, copies):
        for d in range(1, nc):
            peer = after(c, d, nc)
            copies.put(
                ref.gs.at[0:ng, at(peer * 32, 32, 8)], ref.rgc.at[h, d - 1, 0:ng],
                ref.gc_s.at[d - 1], ref.gc_r.at[h, d - 1], {"tok_2": peer},
            )

    def gram_to_y(h, ng, copies):
        value = ref.gs[0:ng, at(c * 32, 32, 8), :]
        for d in range(1, nc):
            copies.arrived(
                ref.rgc.at[h, d - 1, 0:ng], ref.gc_s.at[d - 1], ref.gc_r.at[h, d - 1],
                {"tok_2": before(c, d, nc)},
            )
            value = value + ref.rgc[h, d - 1, 0:ng]
        ref.gy[0:ng] = value
        for d in range(1, ny):
            peer = after(y, d, ny)
            copies.put(
                ref.gy.at[0:ng, at(peer * 8, 8, 8)], ref.rgy.at[h, d - 1, 0:ng],
                ref.gy_s.at[d - 1], ref.gy_r.at[h, d - 1], {"tok_0": peer},
            )

    def gram_to_z(h, ng, copies):
        value = ref.gy[0:ng, at(y * 8, 8, 8), :]
        for d in range(1, ny):
            copies.arrived(
                ref.rgy.at[h, d - 1, 0:ng], ref.gy_s.at[d - 1], ref.gy_r.at[h, d - 1],
                {"tok_0": before(y, d, ny)},
            )
            value = value + ref.rgy[h, d - 1, 0:ng]
        ref.gz[0:ng] = value
        for d in range(1, nz):
            copies.put(
                ref.gz.at[0:ng], ref.rgz.at[h, d - 1, 0:ng],
                ref.gz_s.at[d - 1], ref.gz_r.at[h, d - 1], {"tok_1": after(z, d, nz)},
            )

    def gram_to_all(h, ng, copies):
        value = ref.gz[0:ng]
        for d in range(1, nz):
            copies.arrived(
                ref.rgz.at[h, d - 1, 0:ng], ref.gz_s.at[d - 1], ref.gz_r.at[h, d - 1],
                {"tok_1": before(z, d, nz)},
            )
            value = value + ref.rgz[h, d - 1, 0:ng]
        mine = place(x, y, c)
        ref.gm[0:ng] = value
        ref.ga[h, mine, 0:ng] = value
        for i, d in enumerate(plane):
            copies.put(
                ref.gm.at[0:ng], ref.ga.at[h, mine, 0:ng],
                ref.ga_s.at[i], ref.ga_r.at[h, i], on_plane(*d)[1],
            )

    def gram_whole(h, ng, copies):
        for i, (dx, dy, dc) in enumerate(plane):
            where, device = on_plane(-dx, -dy, -dc)
            copies.arrived(
                ref.ga.at[h, place(*where), 0:ng], ref.ga_s.at[i], ref.ga_r.at[h, i], device
            )
        for g in range(nx * ny * nc):
            for n in range(ng):
                ref.gram[n, g * 8 : g * 8 + 8, :] = ref.ga[h, g, n]

    def half_step(h, carry):
        copies = Copies()
        side = lax.rem(h, 2)
        source, target = ref.acts.at[1 - side], ref.acts.at[side]
        zf = ref.z.at[h]
        opening = h == 0

        @pl.when(opening)
        def _():
            loads[0].wait()
            loads[1].wait()

        def beside():
            @pl.when(opening)
            def _():
                loads[2].wait()
                column_sums()

        projected(h, source, zf, copies, opening, beside)
        for i in range(2):
            ref.zt[i * 128 : i * 128 + 128, :] = zf[i].T
        gram_rows(zf, [ref.zt[at(x * 64, 64, 16), :]])
        gram_to_core(h, 1, copies)
        for lo in range(0, feats, 256):
            hi = min(lo + 256, feats)
            ref.cb[lo:hi, :] = jnp.dot(ref.zt[...], target[:, lo:hi], preferred_element_type=F32).T
        for d in range(1, nc):
            peer = after(c, d, nc)
            rows = at(peer * per_c, per_c, PIECE)
            copies.put(
                ref.cb.at[rows], ref.rcc.at[h, d - 1],
                ref.cc_s.at[d - 1], ref.cc_r.at[h, d - 1], {"tok_2": peer},
            )
            copies.put(
                ref.sb.at[rows], ref.rsc.at[d - 1],
                ref.sc_s.at[d - 1], ref.sc_r.at[d - 1], {"tok_2": peer}, opening,
            )
        gram_to_y(h, 1, copies)

        own = at(c * per_c, per_c, PIECE)
        value = ref.cb[own, :]
        for d in range(1, nc):
            copies.arrived(
                ref.rcc.at[h, d - 1], ref.cc_s.at[d - 1], ref.cc_r.at[h, d - 1],
                {"tok_2": before(c, d, nc)},
            )
            value = value + ref.rcc[h, d - 1]
        ref.cy[...] = value
        for d in range(1, ny):
            peer = after(y, d, ny)
            copies.put(
                ref.cy.at[at(peer * per_y, per_y, PIECE)], ref.rcy.at[h, d - 1],
                ref.cy_s.at[d - 1], ref.cy_r.at[h, d - 1], {"tok_0": peer},
            )

        @pl.when(opening)
        def _():
            sums = ref.sb[own, :]
            for d in range(1, nc):
                copies.arrived(
                    ref.rsc.at[d - 1], ref.sc_s.at[d - 1], ref.sc_r.at[d - 1],
                    {"tok_2": before(c, d, nc)},
                )
                sums = sums + ref.rsc[d - 1]
            ref.sy[...] = sums

        for d in range(1, ny):
            peer = after(y, d, ny)
            copies.put(
                ref.sy.at[at(peer * per_y, per_y, PIECE)], ref.rsy.at[d - 1],
                ref.sy_s.at[d - 1], ref.sy_r.at[d - 1], {"tok_0": peer}, opening,
            )
        gram_to_z(h, 1, copies)
        own = at(y * per_y, per_y, PIECE)
        value = ref.cy[own, :]
        for d in range(1, ny):
            copies.arrived(
                ref.rcy.at[h, d - 1], ref.cy_s.at[d - 1], ref.cy_r.at[h, d - 1],
                {"tok_0": before(y, d, ny)},
            )
            value = value + ref.rcy[h, d - 1]
        ref.cz[...] = value

        def to_owner(peer):
            return at(lax.rem(peer, owners) * PIECE, PIECE, PIECE)

        for d in range(1, nz):
            peer = after(z, d, nz)
            copies.put(
                ref.cz.at[to_owner(peer)], ref.rcz.at[h, d - 1],
                ref.cz_s.at[d - 1], ref.cz_r.at[h, d - 1], {"tok_1": peer}, peer < owners,
            )

        @pl.when(opening)
        def _():
            sums = ref.sy[own, :]
            for d in range(1, ny):
                copies.arrived(
                    ref.rsy.at[d - 1], ref.sy_s.at[d - 1], ref.sy_r.at[d - 1],
                    {"tok_0": before(y, d, ny)},
                )
                sums = sums + ref.rsy[d - 1]
            ref.sz[...] = sums

        for d in range(1, nz):
            peer = after(z, d, nz)
            copies.put(
                ref.sz.at[to_owner(peer)], ref.rsz.at[d - 1],
                ref.sz_s.at[d - 1], ref.sz_r.at[d - 1], {"tok_1": peer}, opening & (peer < owners),
            )
        gram_to_all(h, 1, copies)

        owner = z < owners
        wf = ref.wf.at[h]
        row = c * per_c + y * per_y
        mine = at(row + lax.rem(z, owners) * PIECE, PIECE, PIECE)

        @pl.when(opening & owner)
        def _():
            sums = ref.sz[to_owner(z), :]
            for d in range(1, nz):
                copies.arrived(
                    ref.rsz.at[d - 1], ref.sz_s.at[d - 1], ref.sz_r.at[d - 1],
                    {"tok_1": before(z, d, nz)},
                )
                sums = sums + ref.rsz[d - 1]
            ref.ss[...] = sums

        @pl.when(owner)
        def _():
            value = ref.cz[to_owner(z), :]
            for d in range(1, nz):
                copies.arrived(
                    ref.rcz.at[h, d - 1], ref.cz_s.at[d - 1], ref.cz_r.at[h, d - 1],
                    {"tok_1": before(z, d, nz)},
                )
                value = value + ref.rcz[h, d - 1]
            sums = jnp.where(side == 0, ref.ss[:, 0:1], ref.ss[:, 64:65])
            value = (value * count) * (root / (sums * count + 0.5))
            ref.pc[...] = value
            wf[mine, :] = value

        for d in range(1, nz):
            copies.put(
                ref.pc, wf.at[mine], ref.wz_s.at[d - 1], ref.wz_r.at[h, d - 1],
                {"tok_1": after(z, d, nz)}, owner,
            )
        for d in range(1, nz):
            sender = before(z, d, nz)
            copies.arrived(
                wf.at[at(row + lax.rem(sender, owners) * PIECE, PIECE, PIECE)],
                ref.wz_s.at[d - 1], ref.wz_r.at[h, d - 1], {"tok_1": sender}, sender < owners,
            )
        for d in range(1, ny):
            mine = at(row, per_y, PIECE)
            copies.put(
                wf.at[mine], wf.at[mine], ref.wy_s.at[d - 1], ref.wy_r.at[h, d - 1],
                {"tok_0": after(y, d, ny)},
            )
        gram_whole(h, 1, copies)

        def between():
            for d in range(1, ny):
                sender = before(y, d, ny)
                copies.arrived(
                    wf.at[at(c * per_c + sender * per_y, per_y, PIECE)],
                    ref.wy_s.at[d - 1], ref.wy_r.at[h, d - 1], {"tok_0": sender},
                )
            for d in range(1, nc):
                mine = at(c * per_c, per_c, PIECE)
                copies.put(
                    wf.at[mine], wf.at[mine], ref.wc_s.at[d - 1], ref.wc_r.at[h, d - 1],
                    {"tok_2": after(c, d, nc)},
                )

        inverse_into(ref.gram.at[0], count, ref.inv, between)
        for d in range(1, nc):
            sender = before(c, d, nc)
            copies.arrived(
                wf.at[at(sender * per_c, per_c, PIECE)],
                ref.wc_s.at[d - 1], ref.wc_r.at[h, d - 1], {"tok_2": sender},
            )
        high_inv, low_inv = split(ref.inv[...])
        for lo in range(0, feats, feats // 4):
            rows = slice(lo, lo + feats // 4)
            high_w, low_w = split(wf[rows, :])
            value = mm(high_w, low_inv, 1, 1, None) + mm(low_w, high_inv, 1, 1, None)
            ref.w[rows, :] = (value + mm(high_w, high_inv, 1, 1, None)).astype(BF16)

        @pl.when(h == STEPS - 2)
        def _():
            ref.first_dirs[...] = ref.w[...]

        @pl.when(h == STEPS - 1)
        def _():
            ref.second_dirs[...] = ref.w[...]

        copies.drain()
        return carry

    lax.fori_loop(0, STEPS, half_step, 0)

    h = STEPS
    copies = Copies()
    zf = ref.z.at[h]
    projected(h, ref.acts.at[1], zf, copies, None, lambda: None)
    before_rows = ref.zt[at(x * 64, 64, 16), :]
    for i in range(2):
        ref.zl[i * 128 : i * 128 + 128, :] = zf[i].T
    gram_rows(zf, [ref.zl[at(x * 64, 64, 16), :], before_rows])
    gram_to_core(h, 2, copies)
    gram_to_y(h, 2, copies)
    gram_to_z(h, 2, copies)
    gram_to_all(h, 2, copies)
    gram_whole(h, 2, copies)
    left = mm(ref.inv[...], ref.gram[1] * count)
    inverse_into(ref.gram.at[0], count, ref.last)
    ref.correlation[...] = mm(left, ref.last[...], 1, 1)
    copies.drain()


def body(first_acts, second_acts, start_dirs):
    nx, ny, nz, nc = (lax.axis_size(a) for a in ("feat", *TOK))
    tokens, feats = first_acts.shape
    k = start_dirs.shape[1]
    per_y = (nz - 1) * PIECE
    per_c = ny * per_y
    assert per_c * nc == feats and nx == 4 and k == 256 and ny * nc == 8
    total = float(tokens * ny * nz * nc)
    root = float(feats * nx) ** 0.5
    vmem, hbm = pl.BlockSpec(memory_space=pltpu.VMEM), pl.BlockSpec(memory_space=pl.ANY)
    chunk = tokens // CHUNKS
    every = STEPS + 1
    parts = 2 * CHUNKS
    members = nx * ny * nc

    def f32(*shape):
        return pltpu.VMEM(shape, F32)

    def bf16(*shape):
        return pltpu.VMEM(shape, BF16)

    def dma(*shape):
        return pltpu.SemaphoreType.DMA(shape)

    ins = ["first_acts", "second_acts", "start_dirs"]
    outs = dict(
        first_dirs=jax.ShapeDtypeStruct((feats, k), BF16),
        second_dirs=jax.ShapeDtypeStruct((feats, k), BF16),
        correlation=jax.ShapeDtypeStruct((k, k), F32),
    )
    scratch = dict(
        acts=bf16(2, tokens, feats), load_sem=dma(3), w=bf16(feats, k),
        part=f32(tokens, k), out=bf16(2, tokens, 128), z=bf16(every, 2, tokens, 128),
        zt=bf16(k, tokens), zl=bf16(k, tokens),
        r1=bf16(every, parts, chunk // 2, 128), g2=bf16(parts, chunk // 4, 128),
        r2=bf16(every, parts, chunk // 4, 128), x_s=dma(parts, 4), x_r=dma(every, parts, 4),
        gs=f32(2, 64, k), rgc=f32(every, nc - 1, 2, 32, k), gc_s=dma(nc - 1), gc_r=dma(every, nc - 1),
        gy=f32(2, 32, k), rgy=f32(every, ny - 1, 2, 8, k), gy_s=dma(ny - 1), gy_r=dma(every, ny - 1),
        gz=f32(2, 8, k), rgz=f32(every, nz - 1, 2, 8, k), gz_s=dma(nz - 1), gz_r=dma(every, nz - 1),
        gm=f32(2, 8, k), ga=f32(every, members, 2, 8, k), ga_s=dma(members - 1),
        ga_r=dma(every, members - 1), gram=f32(2, k, k), inv=f32(k, k), last=f32(k, k),
        cb=f32(feats, k), rcc=f32(STEPS, nc - 1, per_c, k), cc_s=dma(nc - 1), cc_r=dma(STEPS, nc - 1),
        cy=f32(per_c, k), rcy=f32(STEPS, ny - 1, per_y, k), cy_s=dma(ny - 1), cy_r=dma(STEPS, ny - 1),
        cz=f32(per_y, k), rcz=f32(STEPS, nz - 1, PIECE, k), cz_s=dma(nz - 1), cz_r=dma(STEPS, nz - 1),
        sb=f32(feats, 128), rsc=f32(nc - 1, per_c, 128), sc_s=dma(nc - 1), sc_r=dma(nc - 1),
        sy=f32(per_c, 128), rsy=f32(ny - 1, per_y, 128), sy_s=dma(ny - 1), sy_r=dma(ny - 1),
        sz=f32(per_y, 128), rsz=f32(nz - 1, PIECE, 128), sz_s=dma(nz - 1), sz_r=dma(nz - 1),
        ss=f32(PIECE, 128), pc=f32(PIECE, k), wf=f32(STEPS, feats, k),
        wz_s=dma(nz - 1), wz_r=dma(STEPS, nz - 1), wy_s=dma(ny - 1), wy_r=dma(STEPS, ny - 1),
        wc_s=dma(nc - 1), wc_r=dma(STEPS, nc - 1),
    )
    names = [*ins, *outs, *scratch]
    return pl.pallas_call(
        functools.partial(kernel, names, total, root),
        out_shape=tuple(outs.values()),
        in_specs=[hbm, hbm, hbm],
        out_specs=(vmem, vmem, vmem),
        scratch_shapes=list(scratch.values()),
        compiler_params=pltpu.CompilerParams(
            collective_id=0, has_side_effects=True, vmem_limit_bytes=60 << 20
        ),
        name="cca",
    )(first_acts, second_acts, start_dirs)


def solution(mesh):
    split_mesh = Mesh(
        mesh.devices.reshape(4, 8, 2, mesh.shape["feat"]), ("tok_0", "tok_1", "tok_2", "feat")
    )
    in_specs = (P(TOK, "feat"), P(TOK, "feat"), P("feat", None))
    out_specs = (P("feat", None), P("feat", None), P())
    return jax.shard_map(
        body, mesh=split_mesh, in_specs=in_specs, out_specs=out_specs, check_vma=False
    )
```
